32 devices in a mesh: groups: 2 (over y), wide: 4 (over z), narrow: 4 (over x, core).
Axes of the slice: x: 2, y: 2, z: 4, core: 2. Of those that a mesh axis runs over, the one named last changes fastest.
Arguments:
- cont_queries: bfloat16 [32, 128, 64, 128], P(('groups', 'wide'), None, 'narrow'), parts along dimension 0, may hold values from -5 to 5
- cont_keys: bfloat16 [32, 128, 8, 128], P(('groups', 'wide'), None, 'narrow'), parts along dimension 0, may hold values from -5 to 5
- cont_values: bfloat16 [32, 128, 8, 128], P(('groups', 'wide'), None, 'narrow'), parts along dimension 0, may hold values from -5 to 5
- prefix_kv: bfloat16 [8, 2, 128, 8, 128], P(('groups', 'wide'), None, None, 'narrow'), parts along dimension 0, may hold values from -5 to 5
- probe: bfloat16 [64, 128], P('narrow'), may hold values from -0.5 to 0.5
- question_row: int32 [8], P('groups'), parts along dimension 0, may hold values from 0 to 3, each once
- cont_slot: int32 [32], P(('groups', 'wide')), parts along dimension 0, may hold values from 0 to 15, each once
- cont_length: int32 [32], P(('groups', 'wide')), parts along dimension 0, may hold values from 1 to 128
- gold: int32 [8], P('groups'), parts along dimension 0, may hold values from 0 to 3
Outputs:
- token_score: float32 [32, 128], P(('groups', 'wide')), parts along dimension 0
- owned_logprob: float32 [8, 4], P(('groups', 'wide')), parts along dimension 0
- owned_loss: float32 [8], P(('groups', 'wide')), parts along dimension 0
The draws below stay inside these ranges and needn't reach their ends.
There are 2 independent parts, one for each index of `groups`. The reference program is written for one: setup_inputs(seed, part) draws one part's arguments, and reference() takes and returns one part's arrays. A program takes and returns all parts, laid end to end along the dimension named above; an argument that names none is the same for every part. Nothing has to cross between parts.
All inputs are finite; a program needn't handle non-finite values.
Results may differ from the reference program's by a relative error of at most 0.0065.
Values may be sent and summed in bfloat16 or wider, within the bound.
A program may use at most 64 MiB of HBM per device.

```python
import jax
import jax.numpy as jnp
from jax import lax

HEADS = 64
KV_HEADS = 8
HEAD_DIM = 128
ANSWERS = 4
CLEN = 128
PREF = 128
QUESTIONS = 4
CONTS = 16


def draw_cont_queries(key, part):
    drawn = jax.random.normal(jax.random.fold_in(key, 1), (CONTS, CLEN, HEADS, HEAD_DIM), jnp.float32)
    drawn = jnp.clip(drawn, -5.0, 5.0)
    return drawn.astype(jnp.bfloat16)


def draw_prefix_kv(key, part):
    drawn = jax.random.normal(jax.random.fold_in(key, 2), (QUESTIONS, 2, PREF, KV_HEADS, HEAD_DIM), jnp.float32)
    drawn = jnp.clip(drawn, -5.0, 5.0)
    return drawn.astype(jnp.bfloat16)


def plant(values, rng, least, top_value):
    dims = values.shape
    index_at = [jax.random.randint(jax.random.fold_in(rng, axis), (), 0, dims[axis]) for axis in range(len(dims))]
    values = values.at[tuple(index_at)].set(least)
    longest = dims.index(max(dims))
    index_at[longest] = (index_at[longest] + 1) % dims[longest]
    return values.at[tuple(index_at)].set(top_value)


def steps_of(own_key, dims, cuts, low, top_value):
    gain = 1.0
    for dim, blocks in cuts:
        steps = jax.random.uniform(jax.random.fold_in(jax.random.fold_in(own_key, 6), dim), (blocks,), jnp.float32, low / len(cuts), top_value / len(cuts))
        gain = gain * jnp.repeat(jnp.exp(steps), dims[dim] // blocks).reshape((-1,) + (1,) * (len(dims) - 1 - dim))
    return gain


def noise(own_key, shape, spread, limit, split=(), held_as=jnp.bfloat16):
    result = jax.random.normal(own_key, shape, jnp.float32) * spread
    if len(split) > 0:
        result = steps_of(own_key, shape, split, -0.22, 0.18) * result
    return jnp.clip(result, min=-limit, max=limit).astype(held_as)


def setup_inputs(seed: int = 0, part: int = 0) -> dict:
    key_list = jax.random.split(jax.random.key(seed), 10)
    own_keys = jax.random.split(jax.random.fold_in(key_list[9], part), 10)
    return {
        "cont_queries": draw_cont_queries(jax.random.fold_in(jax.random.fold_in(key_list[9], part), 71), part),
        "cont_keys": noise(own_keys[1], (CONTS, CLEN, KV_HEADS, HEAD_DIM), 1.0, 5.0, ((0, 4), (2, 4))),
        "cont_values": noise(own_keys[2], (CONTS, CLEN, KV_HEADS, HEAD_DIM), 1.0, 5.0, ((0, 4), (2, 4))),
        "prefix_kv": draw_prefix_kv(jax.random.fold_in(jax.random.fold_in(key_list[9], part), 71), part),
        "probe": noise(key_list[4], (HEADS, HEAD_DIM), HEAD_DIM ** -0.5, 0.5, ((0, 4),)),
        "question_row": jax.random.permutation(own_keys[5], QUESTIONS).astype(jnp.int32),
        "cont_slot": jax.random.permutation(own_keys[6], CONTS).astype(jnp.int32),
        "cont_length": plant(jax.random.randint(own_keys[7], (CONTS,), 1, CLEN + 1), jax.random.fold_in(own_keys[7], 1), 1, CLEN).astype(jnp.int32),
        "gold": plant(jax.random.randint(own_keys[8], (QUESTIONS,), 0, ANSWERS), jax.random.fold_in(own_keys[8], 1), 0, ANSWERS - 1).astype(jnp.int32),
    }


def reference(cont_queries, cont_keys, cont_values, prefix_kv, probe, question_row, cont_slot, cont_length, gold):
    group_size = HEADS // KV_HEADS
    scale_factor = 1.0 / (HEAD_DIM ** 0.5)
    wanted = question_row[cont_slot // ANSWERS].astype(jnp.int32)
    causal = jnp.arange(CLEN)[:, None] >= jnp.arange(CLEN)[None, :]
    allowed = jnp.concatenate([jnp.ones((CLEN, PREF), dtype=bool), causal], axis=1)

    def score_one(packed):
        queries, keys_own, values_own, prefix_row = packed
        cached = lax.dynamic_index_in_dim(prefix_kv, prefix_row, 0, keepdims=False)
        keys_all = jnp.concatenate([cached[0], keys_own], axis=0)
        values_all = jnp.concatenate([cached[1], values_own], axis=0)
        keys_wide = jnp.repeat(keys_all, group_size, axis=1).astype(jnp.float32)
        values_wide = jnp.repeat(values_all, group_size, axis=1).astype(jnp.float32)
        scores = jnp.einsum("thd,jhd->htj", queries.astype(jnp.float32), keys_wide) * scale_factor
        scores = jnp.where(allowed[None, :, :], scores, -jnp.inf)
        row_max = jnp.max(scores, axis=-1, keepdims=True)
        expo = jnp.exp(scores - row_max)
        total = jnp.sum(expo, axis=-1)
        weights = expo.astype(jnp.bfloat16)
        summed = jnp.einsum("htj,jhd->thd", weights.astype(jnp.float32), values_wide)
        attended = (summed / jnp.transpose(total)[:, :, None]).astype(jnp.bfloat16)
        return jnp.einsum("thd,hd->t", attended.astype(jnp.float32), probe.astype(jnp.float32))

    token_score = lax.map(score_one, (cont_queries, cont_keys, cont_values, wanted))
    valid = jnp.arange(CLEN)[None, :] < cont_length[:, None]
    choice_score = jnp.sum(jnp.where(valid, token_score, jnp.zeros_like(token_score)), axis=1)
    question_score = jnp.zeros((QUESTIONS * ANSWERS,), jnp.float32).astype(choice_score.dtype)
    question_score = question_score.at[cont_slot].set(choice_score).reshape(QUESTIONS, ANSWERS)
    logprob = question_score - jax.nn.logsumexp(question_score, axis=1, keepdims=True)
    owned_logprob = jnp.zeros_like(logprob).at[question_row].set(logprob)
    picked = jnp.take_along_axis(logprob, gold[:, None].astype(jnp.int32), axis=1)[:, 0]
    owned_loss = jnp.zeros_like(picked).at[question_row].set(-picked)
    return token_score, owned_logprob, owned_loss
```

```python
import functools

import jax
import jax.numpy as jnp
from jax import lax
from jax.experimental import pallas as pl
from jax.experimental.pallas import tpu as pltpu
from jax.sharding import PartitionSpec as P

MESH = pl.DeviceIdType.MESH
ANSWERS = 4
LANES = 128
NEG = -1e30
LOG2E = 1.4426950408889634
F32 = jnp.float32
BF16 = jnp.bfloat16
NT = (((1,), (1,)), ((), ()))
TN = (((0,), (0,)), ((), ()))


def iota(shape, dim):
    return lax.broadcasted_iota(jnp.int32, shape, dim)


def kernel(
    sizes,
    qrow_hbm, slot_hbm, len_hbm, gold_hbm, q_hbm, k_hbm, v_hbm, pre_hbm, probe_hbm,
    out_ref,
    qrow_ref, slot_ref, len_ref, gold_ref, probe_ref, q2_v,
    q_v, k_v, v_v, pv_v, kslot, vpslot, split, kown, vpt, kpre, vptp,
    m1, l1, n1, m2, l2, n2, tslot, cbuf, cslot,
    in_sem, send_sem, recv_sem,
):
    wide, narrow, conts, clen, heads, kv, dim, quest, pref, questions = sizes
    group = heads // kv
    scale = LOG2E / dim**0.5
    me_w = lax.axis_index("wide")
    me_n = lax.axis_index("narrow")
    tcols = 2 * LANES // heads
    cols = tcols * heads
    blocks = clen // tcols
    own = pl.ds(me_w * quest, quest)

    cp_k = pltpu.make_async_copy(pre_hbm.at[:, 0], kslot.at[own], in_sem.at[0])
    cp_v = pltpu.make_async_copy(pre_hbm.at[:, 1], pv_v, in_sem.at[1])
    cp_ko = pltpu.make_async_copy(k_hbm, k_v, in_sem.at[2])
    cp_vo = pltpu.make_async_copy(v_hbm, v_v, in_sem.at[3])
    cp_q = pltpu.make_async_copy(q_hbm, q_v, in_sem.at[4])
    cp_p = pltpu.make_async_copy(probe_hbm, probe_ref, in_sem.at[5])
    scalars = [
        pltpu.make_async_copy(src, dst, in_sem.at[6 + i])
        for i, (src, dst) in enumerate(
            ((qrow_hbm, qrow_ref), (slot_hbm, slot_ref), (len_hbm, len_ref), (gold_hbm, gold_ref))
        )
    ]
    for cp in (cp_k, cp_v, cp_p, cp_ko, cp_vo, cp_q, *scalars):
        cp.start()

    total = wide * narrow
    me = me_w * narrow + me_n
    far = sorted(range(1, wide), key=lambda i: (-min(i, wide - i), i))
    wides = [lax.rem(me_w + i, wide) for i in range(wide)]
    narrows = [lax.rem(me_n + i, narrow) for i in range(narrow)]

    barrier = pltpu.get_barrier_semaphore()
    near = [{"wide": wides[i]} for i in far] + [{"narrow": to} for to in narrows[1:]]
    for to in near:
        pl.semaphore_signal(barrier, inc=1, device_id=to, device_id_type=MESH)
    pl.semaphore_wait(barrier, len(near))

    def remote(src, dst, n, to):
        return pltpu.make_async_remote_copy(
            src_ref=src, dst_ref=dst, send_sem=send_sem.at[n], recv_sem=recv_sem.at[n],
            device_id=to, device_id_type=MESH,
        )

    def share(buf, n):
        for i in far:
            remote(buf.at[own], buf.at[own], n, {"wide": wides[i]}).start()

    def drained(buf, n, count):
        part = buf.at[pl.ds(0, count)]
        return remote(part, part, n, {"wide": wides[1]})

    cp_k.wait()
    share(kslot, 0)

    cp_p.wait()
    probe = probe_ref[...]
    lane = iota((1, LANES), 1)
    lane_kv = (lane % heads) // group
    rowsel = iota((LANES, heads), 0) % heads == iota((LANES, heads), 1)
    tile_mat = jnp.where(rowsel, 1.0, 0.0).astype(BF16)
    probe_t = lax.dot_general(
        tile_mat, probe, (((1,), (0,)), ((), ())), preferred_element_type=F32
    ).astype(BF16)
    expand = jnp.where(iota((heads, LANES), 1) % heads == iota((heads, LANES), 0), 1.0, 0.0)

    def unpack(x):
        split[...] = x.astype(F32)
        n = x.shape[0] // kv
        return [split[pl.ds(i, n, stride=kv), :] for i in range(kv)]

    cp_v.wait()
    head_kv = iota((heads, 1), 0) // group
    for r in range(quest):
        acc = jnp.zeros((heads, pref), F32)
        for i, part in enumerate(unpack(pv_v[r])):
            d = lax.dot_general(probe, part.astype(BF16), NT, preferred_element_type=F32)
            acc = jnp.where(head_kv == i, d, acc)
        vpslot[me_w * quest + r] = acc
    share(vpslot, 1)

    def start_mask(c, b):
        rows = q_v[c, pl.ds(b * cols, cols), :]
        rk = (iota((cols, 1), 0) % heads) // group
        return jnp.concatenate(
            [rows * jnp.where(rk == i, 1.0, 0.0).astype(BF16) for i in range(kv)], axis=1
        )

    def softmax_part(s, vp):
        m = jnp.max(s, axis=0, keepdims=True)
        e = jnp.exp2((s - m) * scale)
        l = jnp.sum(e, axis=0, keepdims=True)
        n = jnp.sum(e * jnp.concatenate([vp] * (cols // LANES), axis=1), axis=0, keepdims=True)
        return m, l, n

    cp_ko.wait()
    cp_vo.wait()
    cp_q.wait()
    block_id = iota((blocks, cols), 0)

    def gather(stats, b, news):
        return [jnp.where(block_id == b, new, old) for new, old in zip(news, stats)]

    blank = jnp.zeros((blocks, cols), F32)

    def own_part(c, _):
        parts = unpack(k_v[c])
        for i in range(kv):
            kown[:, i * dim:(i + 1) * dim] = parts[i].astype(BF16)
        d = lax.dot_general(v_v[c], probe_t, NT, preferred_element_type=F32)
        split[...] = d
        acc = split[pl.ds(0, clen, stride=kv), :]
        for i in range(1, kv):
            acc = jnp.where(lane_kv == i, split[pl.ds(i, clen, stride=kv), :], acc)
        vpt[...] = acc
        stats = [blank] * 3
        for b in range(blocks):
            n_rows = (b + 1) * tcols
            q2 = start_mask(c, b)
            q2_v[c, pl.ds(b * cols, cols), :] = q2
            s = lax.dot_general(kown[:n_rows, :], q2, NT, preferred_element_type=F32)
            ok = iota((tcols, cols), 0) <= iota((tcols, cols), 1) // heads
            last = jnp.where(ok, s[n_rows - tcols:], NEG)
            s = last if b == 0 else jnp.concatenate([s[:n_rows - tcols], last], axis=0)
            m, l, n = softmax_part(s, vpt[:n_rows, :])
            stats = gather(stats, b, (m, l, n))
        m1[c], l1[c], n1[c] = stats
        return 0

    lax.fori_loop(0, conts, own_part, 0)

    others = (wide - 1) * quest
    for n, buf in ((0, kslot), (1, vpslot)):
        drained(buf, n, others).wait_recv()
        drained(buf, n, others).wait_send()

    for cp in scalars:
        cp.wait()

    def prefix_part(c, _):
        w = qrow_ref[slot_ref[c] // ANSWERS]
        parts = unpack(kslot[w])
        for i in range(kv):
            kpre[:, i * dim:(i + 1) * dim] = parts[i].astype(BF16)
        vptp[...] = lax.dot_general(
            vpslot[w], expand, TN, preferred_element_type=F32, precision=lax.Precision.HIGHEST
        )
        stats = [blank] * 3
        for b in range(blocks):
            q2 = q2_v[c, pl.ds(b * cols, cols), :]
            s = lax.dot_general(kpre[...], q2, NT, preferred_element_type=F32)
            m, l, n = softmax_part(s, vptp[...])
            stats = gather(stats, b, (m, l, n))
        m2[c], l2[c], n2[c] = stats
        return 0

    lax.fori_loop(0, conts, prefix_part, 0)

    fold = jnp.where(iota((cols, clen), 0) // heads == iota((cols, clen), 1) % tcols, 1.0, 0.0)
    keep = iota((blocks, clen), 1) // tcols == iota((blocks, clen), 0)
    row_id = iota((conts, clen), 0)
    partial = jnp.zeros((conts, clen), F32)
    for c in range(conts):
        ma, mb = m1[c], m2[c]
        m = jnp.maximum(ma, mb)
        ea, eb = jnp.exp2((ma - m) * scale), jnp.exp2((mb - m) * scale)
        ratio = (n1[c] * ea + n2[c] * eb) / (l1[c] * ea + l2[c] * eb)
        y = jnp.dot(ratio, fold, preferred_element_type=F32, precision=lax.Precision.HIGHEST)
        y = jnp.sum(jnp.where(keep, y, 0.0), axis=0, keepdims=True)
        partial = jnp.where(row_id == c, y, partial)
    tslot[me_n] = partial

    choice_rows = wide * quest
    crow = iota((wide, quest, LANES), 0) * quest + iota((wide, quest, LANES), 1)
    clane = iota((wide, quest, LANES), 2)
    term = jnp.zeros((wide, quest, LANES), F32)
    tpos = iota((1, clen), 1)
    for c in range(conts):
        slot = slot_ref[c]
        w = qrow_ref[slot // ANSWERS]
        a = slot % ANSWERS
        val = jnp.sum(jnp.where(tpos < len_ref[c], partial[c:c + 1, :], 0.0), axis=1, keepdims=True)
        term = term + jnp.where((crow == w) & (clane == a), val.reshape(1, 1, 1), 0.0)
    cbuf[...] = term

    def hand(i, j):
        to = {"wide": wides[i], "narrow": narrows[j]}
        remote(cbuf.at[wides[i]], cslot.at[me], 2, to).start()

    if total <= 16:
        for j in range(narrow - 1, -1, -1):
            for i in (*far, 0):
                if i or j:
                    hand(i, j)
    else:
        @pl.loop(1, total)
        def _(n):
            p = lax.rem(me + n, total)
            to = {"wide": lax.div(p, narrow), "narrow": lax.rem(p, narrow)}
            remote(cbuf.at[to["wide"]], cslot.at[me], 2, to).start()

    for j in range(1, narrow):
        remote(tslot.at[me_n], tslot.at[me_n], 3, {"narrow": narrows[j]}).start()
    cslot[me] = cbuf[me_w]

    drained(tslot, 3, narrow - 1).wait_recv()
    tok = tslot[0]
    for i in range(1, narrow):
        tok = tok + tslot[i]
    out_ref[0:conts, :] = tok

    drained(cslot, 2, total - 1).wait_recv()
    drained(tslot, 3, narrow - 1).wait_send()
    drained(cslot, 2, total - 1).wait_send()
    scores = jnp.sum(cslot[...], axis=0)
    live = iota((quest, LANES), 1) < ANSWERS
    masked = jnp.where(live, scores, NEG)
    top = jnp.max(masked, axis=1, keepdims=True)
    norm = jnp.log(jnp.sum(jnp.where(live, jnp.exp(masked - top), 0.0), axis=1, keepdims=True))
    logp = scores - top - norm
    out_ref[conts:conts + quest, :] = logp
    mine = me_w * quest + iota((quest, 1), 0)
    gold = jnp.zeros((quest, 1), jnp.int32)
    for g in range(questions):
        gold = jnp.where(mine == qrow_ref[g], gold_ref[g], gold)
    pick = iota((quest, LANES), 1) == gold
    loss = -jnp.sum(jnp.where(pick, logp, 0.0), axis=1, keepdims=True)
    out_ref[conts + quest:conts + 2 * quest, :] = jnp.broadcast_to(loss, (quest, LANES))


def hand_out(conts, quest, packed_ref, tok_ref, logp_ref, loss_ref):
    tok_ref[...] = packed_ref[0:conts, :]
    logp_ref[...] = packed_ref[conts:conts + quest, :ANSWERS]
    loss_ref[...] = packed_ref[conts + quest:conts + 2 * quest, :1]


def solution(mesh):
    wide, narrow = mesh.shape["wide"], mesh.shape["narrow"]
    total = wide * narrow

    def per_device(q, k, v, prefix, probe, qrow, slot, length, gold):
        conts, clen, heads, dim = q.shape
        kv = k.shape[2]
        quest, _, pref = prefix.shape[:3]
        questions = qrow.shape[0]
        cols = 2 * LANES // heads * heads
        blocks = clen * heads // cols
        sizes = (wide, narrow, conts, clen, heads, kv, dim, quest, pref, questions)
        vmem = pl.BlockSpec(memory_space=pltpu.VMEM)
        anyw = pl.BlockSpec(memory_space=pl.ANY)
        stat = pltpu.VMEM((conts, blocks, cols), F32)
        dma = pltpu.SemaphoreType.DMA
        packed = pl.pallas_call(
            functools.partial(kernel, sizes),
            out_shape=pltpu.VMEM((conts + 2 * quest, LANES), F32),
            in_specs=[anyw] * 9,
            out_specs=vmem,
            scratch_shapes=[
                pltpu.SMEM((questions,), jnp.int32),
                pltpu.SMEM((conts,), jnp.int32),
                pltpu.SMEM((conts,), jnp.int32),
                pltpu.SMEM((questions,), jnp.int32),
                pltpu.VMEM((heads, dim), BF16),
                pltpu.VMEM((conts, clen * heads, kv * dim), BF16),
                pltpu.VMEM((conts, clen * heads, dim), BF16),
                pltpu.VMEM((conts, clen * kv, dim), BF16),
                pltpu.VMEM((conts, clen * kv, dim), BF16),
                pltpu.VMEM((quest, pref * kv, dim), BF16),
                pltpu.VMEM((wide * quest, pref * kv, dim), BF16),
                pltpu.VMEM((wide * quest, heads, pref), F32),
                pltpu.VMEM((clen * kv, dim), F32),
                pltpu.VMEM((clen, kv * dim), BF16),
                pltpu.VMEM((clen, LANES), F32),
                pltpu.VMEM((pref, kv * dim), BF16),
                pltpu.VMEM((pref, LANES), F32),
                stat, stat, stat, stat, stat, stat,
                pltpu.VMEM((narrow, conts, clen), F32),
                pltpu.VMEM((wide, quest, LANES), F32),
                pltpu.VMEM((total, quest, LANES), F32),
                dma((10,)),
                dma((4,)), dma((4,)),
            ],
            compiler_params=pltpu.CompilerParams(collective_id=0, has_side_effects=True),
        )(
            qrow, slot, length, gold,
            q.reshape(conts, clen * heads, dim),
            k.reshape(conts, clen * kv, dim),
            v.reshape(conts, clen * kv, dim),
            prefix.reshape(quest, 2, pref * kv, dim),
            probe,
        )
        tok, logp, loss = pl.pallas_call(
            functools.partial(hand_out, conts, quest),
            out_shape=(
                jax.ShapeDtypeStruct((conts, clen), F32),
                jax.ShapeDtypeStruct((quest, ANSWERS), F32),
                jax.ShapeDtypeStruct((quest, 1), F32),
            ),
            in_specs=[vmem],
            out_specs=(vmem, vmem, vmem),
        )(pltpu.with_memory_space_constraint(packed, pltpu.VMEM))
        return tok, logp, loss.reshape(quest)

    return jax.shard_map(
        per_device,
        mesh=mesh,
        in_specs=(
            P(("groups", "wide"), None, "narrow", None),
            P(("groups", "wide"), None, "narrow", None),
            P(("groups", "wide"), None, "narrow", None),
            P(("groups", "wide"), None, None, "narrow", None),
            P("narrow", None),
            P("groups"),
            P(("groups", "wide")),
            P(("groups", "wide")),
            P("groups"),
        ),
        out_specs=(P(("groups", "wide"), None), P(("groups", "wide"), None), P(("groups", "wide"))),
        check_vma=False,
    )
```

```python
import functools

import jax
import jax.numpy as jnp
from jax import lax
from jax.experimental import pallas as pl
from jax.experimental.pallas import tpu as pltpu
from jax.sharding import PartitionSpec as P

MESH = pl.DeviceIdType.MESH
ANSWERS = 4
LANES = 128
SUBLANES = 8
NEG = -1e30
LOG2E = 1.4426950408889634
F32 = jnp.float32
BF16 = jnp.bfloat16
NT = (((1,), (1,)), ((), ()))
TN = (((0,), (0,)), ((), ()))


def iota(shape, dim):
    return lax.broadcasted_iota(jnp.int32, shape, dim)


def kernel(
    sizes,
    qrow_hbm, slot_hbm, len_hbm, gold_hbm, q_hbm, k_hbm, v_hbm, pre_hbm, probe_hbm,
    out_ref,
    qrow_ref, slot_ref, len_ref, gold_ref, probe_ref, qt_v,
    q_v, k_v, v_v, pv_v, kslot_a, kslot_b, vpslot, split, kown, vpt, kpre, vptp,
    ms, ls, ns, tslot, cbuf, cslot,
    in_sem, send_sem, recv_sem, ready, column, everyone,
):
    wide, narrow, conts, clen, heads, kv, dim, quest, pref, questions = sizes
    group = heads // kv
    scale = LOG2E / dim**0.5
    me_w = lax.axis_index("wide")
    me_n = lax.axis_index("narrow")
    tcols = 2 * LANES // heads
    cols = tcols * heads
    blocks = clen // tcols
    own = pl.ds(me_w * quest, quest)

    half = pref // 2
    kslots = (kslot_a, kslot_b)
    cp_ks = [
        pltpu.make_async_copy(
            pre_hbm.at[:, 0, pl.ds(i * half * kv, half * kv)], ref.at[own], in_sem.at[10 * i]
        )
        for i, ref in enumerate(kslots)
    ]
    cp_v = pltpu.make_async_copy(pre_hbm.at[:, 1], pv_v, in_sem.at[1])
    cp_ko = pltpu.make_async_copy(k_hbm, k_v, in_sem.at[2])
    cp_vo = pltpu.make_async_copy(v_hbm, v_v, in_sem.at[3])
    cp_q = pltpu.make_async_copy(q_hbm, q_v, in_sem.at[4])
    cp_p = pltpu.make_async_copy(probe_hbm, probe_ref, in_sem.at[5])
    scalars = [
        pltpu.make_async_copy(src, dst, in_sem.at[6 + i])
        for i, (src, dst) in enumerate(
            ((qrow_hbm, qrow_ref), (slot_hbm, slot_ref), (len_hbm, len_ref), (gold_hbm, gold_ref))
        )
    ]
    for cp in (*cp_ks, cp_v, cp_p, cp_ko, cp_vo, cp_q, *scalars):
        cp.start()

    total = wide * narrow
    me = me_w * narrow + me_n
    far = sorted(range(1, wide), key=lambda i: (-min(i, wide - i), i))
    wides = [lax.rem(me_w + i, wide) for i in range(wide)]
    narrows = [lax.rem(me_n + i, narrow) for i in range(narrow)]
    first = me_w == 0
    patient = first | (lax.rem(me_n, 2) == 1)

    def signal(sem, to):
        pl.semaphore_signal(sem, inc=1, device_id=to, device_id_type=MESH)

    def each(low, high, fn):
        def step(i, _):
            fn(i)
            return 0
        lax.fori_loop(low, high, step, 0)

    def earlier(fn):
        each(0, me_w, fn)

    def later(fn):
        each(me_w + 1, wide, fn)

    barrier = pltpu.get_barrier_semaphore()
    later(lambda p: signal(barrier, {"wide": p}))

    @pl.when(first)
    def _():
        for to in narrows[1:]:
            signal(barrier, {"narrow": to})

    pl.semaphore_wait(barrier, jnp.where(first, narrow - 1, me_w))
    earlier(lambda p: signal(ready.at[me_w], {"wide": p}))

    def remote(src, dst, n, to):
        return pltpu.make_async_remote_copy(
            src_ref=src, dst_ref=dst, send_sem=send_sem.at[n], recv_sem=recv_sem.at[n],
            device_id=to, device_id_type=MESH,
        )

    def share(buf, n):
        return lambda p: remote(buf.at[own], buf.at[own], n, {"wide": p}).start()

    def drained(buf, n, count):
        part = buf.at[pl.ds(0, count)]
        return remote(part, part, n, {"wide": wides[1]})

    cp_ks[0].wait()
    earlier(share(kslot_a, 0))

    cp_p.wait()
    probe = probe_ref[...]
    lane = iota((1, LANES), 1)
    lane_kv = (lane % heads) // group
    rowsel = iota((LANES, heads), 0) % heads == iota((LANES, heads), 1)
    tile_mat = jnp.where(rowsel, 1.0, 0.0).astype(BF16)
    probe_t = lax.dot_general(
        tile_mat, probe, (((1,), (0,)), ((), ())), preferred_element_type=F32
    ).astype(BF16)
    expand = jnp.where(iota((heads, LANES), 1) % heads == iota((heads, LANES), 0), 1.0, 0.0).astype(BF16)

    def unpack(x):
        n = x.shape[0] // kv
        split[0:n * kv] = x.astype(F32)
        return [split[pl.ds(i, n, stride=kv), :] for i in range(kv)]

    cp_v.wait()
    head_kv = iota((heads, 1), 0) // group
    for r in range(quest):
        acc = jnp.zeros((heads, pref), F32)
        for i, part in enumerate(unpack(pv_v[r])):
            d = lax.dot_general(probe, part.astype(BF16), NT, preferred_element_type=F32)
            acc = jnp.where(head_kv == i, d, acc)
        vpslot[me_w * quest + r] = acc.astype(BF16)
    earlier(share(vpslot, 1))

    def meet(p):
        pl.semaphore_wait(ready.at[p], 1)
        share(kslot_a, 0)(p)
        share(vpslot, 1)(p)

    later(meet)
    cp_ks[1].wait()

    def share_rest():
        later(share(kslot_b, 4))
        earlier(share(kslot_b, 4))

    @pl.when(jnp.logical_not(patient))
    def _():
        share_rest()

    @pl.when(first)
    def _():
        for to in narrows[1:]:
            signal(column, {"narrow": to})


    lane_q = (iota((1, cols), 1) % heads) // group
    q_masks = [jnp.where(lane_q == i, 1.0, 0.0).astype(BF16) for i in range(kv)]

    def turn(c, b):
        rows = q_v[c, pl.ds(b * cols, cols), :].T
        return jnp.concatenate([rows * mask for mask in q_masks], axis=0)

    def absorb(s, vp, old=None):
        s = s.reshape(-1, SUBLANES, cols)
        vp = jnp.concatenate([vp] * (cols // LANES), axis=1).reshape(s.shape)
        m = jnp.max(s, axis=0)
        if old is not None:
            m = jnp.maximum(m, old[0])
        e = jnp.exp2((s - m) * scale)
        l = jnp.sum(e, axis=0)
        n = jnp.sum(e * vp, axis=0)
        if old is not None:
            fade = jnp.exp2((old[0] - m) * scale)
            l, n = l + old[1] * fade, n + old[2] * fade
        return m, l, n

    cp_ko.wait()
    cp_vo.wait()
    cp_q.wait()
    def own_part(c, _):
        parts = unpack(k_v[c])
        for i in range(kv):
            kown[:, i * dim:(i + 1) * dim] = parts[i].astype(BF16)
        d = lax.dot_general(v_v[c], probe_t, NT, preferred_element_type=F32)
        split[...] = d
        acc = split[pl.ds(0, clen, stride=kv), :]
        for i in range(1, kv):
            acc = jnp.where(lane_kv == i, split[pl.ds(i, clen, stride=kv), :], acc)
        vpt[...] = acc
        for b in range(blocks):
            n_rows = (b + 1) * tcols
            qt = turn(c, b)
            qt_v[c, b] = qt
            s = jnp.dot(kown[:n_rows, :], qt, preferred_element_type=F32)
            ok = iota((tcols, cols), 0) <= iota((tcols, cols), 1) // heads
            last = jnp.where(ok, s[n_rows - tcols:], NEG)
            s = last if b == 0 else jnp.concatenate([s[:n_rows - tcols], last], axis=0)
            ms[c, b], ls[c, b], ns[c, b] = absorb(s, vpt[:n_rows, :])
        return 0

    lax.fori_loop(0, conts, own_part, 0)

    @pl.when(patient)
    def _():
        share_rest()

    @pl.when(first)
    def _():
        pl.semaphore_wait(column, narrow - 1)
        later(lambda p: signal(everyone, {"wide": p}))

    @pl.when(me_w > 0)
    def _():
        pl.semaphore_wait(everyone, 1)

    others = (wide - 1) * quest
    for cp in scalars:
        cp.wait()
    rows_of = [qrow_ref[slot_ref[c] // ANSWERS] for c in range(conts)]
    drained(vpslot, 1, others).wait_recv()

    def prefix_part(part):
        for c in range(conts):
            for i, x in enumerate(unpack(kslots[part][rows_of[c]])):
                kpre[c, part * half:(part + 1) * half, i * dim:(i + 1) * dim] = x.astype(BF16)
        for c in range(conts):
            keys = pl.ds(part * half, half)
            for b in range(blocks):
                s = jnp.dot(kpre[c, keys], qt_v[c, b], preferred_element_type=F32)
                ms[c, b], ls[c, b], ns[c, b] = absorb(
                    s, vptp[c, keys], (ms[c, b], ls[c, b], ns[c, b])
                )

    for c in range(conts):
        vptp[c] = lax.dot_general(vpslot[rows_of[c]], expand, TN, preferred_element_type=F32)
    drained(kslot_a, 0, others).wait_recv()
    prefix_part(0)
    drained(kslot_b, 4, others).wait_recv()
    prefix_part(1)

    fold = jnp.where(iota((cols, clen), 0) // heads == iota((cols, clen), 1) % tcols, 1.0, 0.0)
    fold = fold.astype(BF16)
    keep = iota((blocks, clen), 1) // tcols == iota((blocks, clen), 0)
    ratios = []
    for c in range(conts):
        m = ms[c]
        fade = jnp.exp2((m - jnp.max(m, axis=1, keepdims=True)) * scale)
        ratios.append(jnp.sum(ns[c] * fade, axis=1) / jnp.sum(ls[c] * fade, axis=1))
    ratio = jnp.concatenate(ratios, axis=0)
    coarse = ratio.astype(BF16)
    fine = (ratio - coarse.astype(F32)).astype(BF16)
    y = jnp.dot(coarse, fold, preferred_element_type=F32)
    y = y + jnp.dot(fine, fold, preferred_element_type=F32)
    y = jnp.where(keep, y.reshape(conts, blocks, clen), 0.0)
    partial = jnp.sum(y, axis=1)
    tslot[me_n] = partial

    tpos = iota((1, clen), 1)
    places = iota((wide, quest * ANSWERS, 1), 0) * (quest * ANSWERS)
    places = places + iota((wide, quest * ANSWERS, 1), 1)
    term = jnp.zeros((wide, quest * ANSWERS, clen), F32)
    for c in range(conts):
        val = jnp.where(tpos < len_ref[c], partial[c:c + 1, :], 0.0)
        place = rows_of[c] * ANSWERS + slot_ref[c] % ANSWERS
        term = jnp.where(places == place, val[None], term)
    cbuf[...] = term

    def hand(i, j):
        to = {"wide": wides[i], "narrow": narrows[j]}
        remote(cbuf.at[wides[i]], cslot.at[me], 2, to).start()

    if total <= 16:
        for j in range(narrow - 1, -1, -1):
            for i in (*far, 0):
                if i or j:
                    hand(i, j)
    else:
        @pl.loop(1, total)
        def _(n):
            p = lax.rem(me + n, total)
            to = {"wide": lax.div(p, narrow), "narrow": lax.rem(p, narrow)}
            remote(cbuf.at[to["wide"]], cslot.at[me], 2, to).start()

    for j in range(1, narrow):
        remote(tslot.at[me_n], tslot.at[me_n], 3, {"narrow": narrows[j]}).start()
    cslot[me] = cbuf[me_w]

    drained(tslot, 3, narrow - 1).wait_recv()
    tok = tslot[0]
    for i in range(1, narrow):
        tok = tok + tslot[i]
    out_ref[0:conts, :] = tok

    drained(cslot, 2, total - 1).wait_recv()
    drained(tslot, 3, narrow - 1).wait_send()
    drained(cslot, 2, total - 1).wait_send()
    for n, buf in ((0, kslot_a), (1, vpslot), (4, kslot_b)):
        drained(buf, n, others).wait_send()
    summed = jnp.sum(jnp.sum(cslot[...], axis=0), axis=1, keepdims=True)
    logps = []
    losses = []
    for r in range(quest):
        score = summed[r * ANSWERS:(r + 1) * ANSWERS]
        top = jnp.max(score, axis=0, keepdims=True)
        norm = jnp.log(jnp.sum(jnp.exp(score - top), axis=0, keepdims=True))
        logp = score - top - norm
        gold = jnp.zeros((1, 1), jnp.int32)
        for g in range(questions):
            gold = jnp.where(me_w * quest + r == qrow_ref[g], gold_ref[g], gold)
        answer = iota((ANSWERS, LANES), 0)
        row = jnp.sum(jnp.where(answer == iota((ANSWERS, LANES), 1), logp, 0.0), axis=0, keepdims=True)
        loss = jnp.sum(jnp.where(answer == gold, -logp, 0.0), axis=0, keepdims=True)
        logps.append(row)
        losses.append(loss)
    for r in range(quest):
        out_ref[conts + r:conts + r + 1, :] = logps[r]
        out_ref[conts + quest + r:conts + quest + r + 1, :] = losses[r]


def hand_out(conts, quest, packed_ref, tok_ref, logp_ref, loss_ref):
    tok_ref[...] = packed_ref[0:conts, :]
    logp_ref[...] = packed_ref[conts:conts + quest, :ANSWERS]
    loss_ref[...] = packed_ref[conts + quest:conts + 2 * quest, :1]


def solution(mesh):
    wide, narrow = mesh.shape["wide"], mesh.shape["narrow"]
    total = wide * narrow

    def per_device(q, k, v, prefix, probe, qrow, slot, length, gold):
        conts, clen, heads, dim = q.shape
        kv = k.shape[2]
        quest, _, pref = prefix.shape[:3]
        questions = qrow.shape[0]
        cols = 2 * LANES // heads * heads
        blocks = clen * heads // cols
        sizes = (wide, narrow, conts, clen, heads, kv, dim, quest, pref, questions)
        vmem = pl.BlockSpec(memory_space=pltpu.VMEM)
        anyw = pl.BlockSpec(memory_space=pl.ANY)
        stat = pltpu.VMEM((conts, blocks, SUBLANES, cols), F32)
        dma = pltpu.SemaphoreType.DMA
        packed = pl.pallas_call(
            functools.partial(kernel, sizes),
            out_shape=pltpu.VMEM((conts + 2 * quest, LANES), F32),
            in_specs=[anyw] * 9,
            out_specs=vmem,
            scratch_shapes=[
                pltpu.SMEM((questions,), jnp.int32),
                pltpu.SMEM((conts,), jnp.int32),
                pltpu.SMEM((conts,), jnp.int32),
                pltpu.SMEM((questions,), jnp.int32),
                pltpu.VMEM((heads, dim), BF16),
                pltpu.VMEM((conts, blocks, kv * dim, cols), BF16),
                pltpu.VMEM((conts, clen * heads, dim), BF16),
                pltpu.VMEM((conts, clen * kv, dim), BF16),
                pltpu.VMEM((conts, clen * kv, dim), BF16),
                pltpu.VMEM((quest, pref * kv, dim), BF16),
                pltpu.VMEM((wide * quest, pref // 2 * kv, dim), BF16),
                pltpu.VMEM((wide * quest, pref // 2 * kv, dim), BF16),
                pltpu.VMEM((wide * quest, heads, pref), BF16),
                pltpu.VMEM((clen * kv, dim), F32),
                pltpu.VMEM((clen, kv * dim), BF16),
                pltpu.VMEM((clen, LANES), F32),
                pltpu.VMEM((conts, pref, kv * dim), BF16),
                pltpu.VMEM((conts, pref, LANES), F32),
                stat, stat, stat,
                pltpu.VMEM((narrow, conts, clen), F32),
                pltpu.VMEM((wide, quest * ANSWERS, clen), F32),
                pltpu.VMEM((total, quest * ANSWERS, clen), F32),
                dma((11,)),
                dma((5,)), dma((5,)),
                pltpu.SemaphoreType.REGULAR((wide,)),
                pltpu.SemaphoreType.REGULAR,
                pltpu.SemaphoreType.REGULAR,
            ],
            compiler_params=pltpu.CompilerParams(collective_id=0, has_side_effects=True),
        )(
            qrow, slot, length, gold,
            q.reshape(conts, clen * heads, dim),
            k.reshape(conts, clen * kv, dim),
            v.reshape(conts, clen * kv, dim),
            prefix.reshape(quest, 2, pref * kv, dim),
            probe,
        )
        tok, logp, loss = pl.pallas_call(
            functools.partial(hand_out, conts, quest),
            out_shape=(
                jax.ShapeDtypeStruct((conts, clen), F32),
                jax.ShapeDtypeStruct((quest, ANSWERS), F32),
                jax.ShapeDtypeStruct((quest, 1), F32),
            ),
            in_specs=[vmem],
            out_specs=(vmem, vmem, vmem),
        )(pltpu.with_memory_space_constraint(packed, pltpu.VMEM))
        return tok, logp, loss.reshape(quest)

    return jax.shard_map(
        per_device,
        mesh=mesh,
        in_specs=(
            P(("groups", "wide"), None, "narrow", None),
            P(("groups", "wide"), None, "narrow", None),
            P(("groups", "wide"), None, "narrow", None),
            P(("groups", "wide"), None, None, "narrow", None),
            P("narrow", None),
            P("groups"),
            P(("groups", "wide")),
            P(("groups", "wide")),
            P("groups"),
        ),
        out_specs=(P(("groups", "wide"), None), P(("groups", "wide"), None), P(("groups", "wide"))),
        check_vma=False,
    )
```

```python
import functools

import jax
import jax.numpy as jnp
from jax import lax
from jax.experimental import pallas as pl
from jax.experimental.pallas import tpu as pltpu
from jax.sharding import PartitionSpec as P

MESH = pl.DeviceIdType.MESH
ANSWERS = 4
LANES = 128
SUBLANES = 8
NEG = -1e30
LOG2E = 1.4426950408889634
F32 = jnp.float32
BF16 = jnp.bfloat16
NT = (((1,), (1,)), ((), ()))
TN = (((0,), (0,)), ((), ()))


def iota(shape, dim):
    return lax.broadcasted_iota(jnp.int32, shape, dim)


def chunks_of(pref):
    out = []
    for share in (2,4,4):
        out.append((sum(size for _, size in out), pref // share))
    return out


def kernel(
    sizes,
    qrow_hbm, slot_hbm, len_hbm, gold_hbm, q_hbm, k_hbm, v_hbm, pre_hbm, probe_hbm,
    out_ref,
    qrow_ref, slot_ref, len_ref, gold_ref, probe_ref, qt_v,
    q_v, k_v, v_v, pv_v, vpslot, split, kown, vpt, kpre, vptp,
    ms, ls, ns, tslot, cbuf, cslot,
    in_sem, send_sem, recv_sem, ready, together, *kslots
):
    wide, narrow, conts, clen, heads, kv, dim, quest, pref, questions = sizes
    group = heads // kv
    scale = LOG2E / dim**0.5
    me_w = lax.axis_index("wide")
    me_n = lax.axis_index("narrow")
    tcols = 2 * LANES // group
    cols = tcols * group
    blocks = clen // tcols
    tiles = [(i, b) for i in range(kv) for b in range(blocks)]
    own = pl.ds(me_w * quest, quest)

    chunks = chunks_of(pref)
    cp_ks = [
        pltpu.make_async_copy(
            pre_hbm.at[:, 0, pl.ds(at * kv, size * kv)], ref.at[own], in_sem.at[10 + i]
        )
        for i, ((at, size), ref) in enumerate(zip(chunks, kslots))
    ]
    cp_v = pltpu.make_async_copy(pre_hbm.at[:, 1], pv_v, in_sem.at[1])
    cp_ko = pltpu.make_async_copy(k_hbm, k_v, in_sem.at[2])
    cp_vo = pltpu.make_async_copy(v_hbm, v_v, in_sem.at[3])
    cp_q = pltpu.make_async_copy(q_hbm, q_v, in_sem.at[4])
    cp_p = pltpu.make_async_copy(probe_hbm, probe_ref, in_sem.at[5])
    scalars = [
        pltpu.make_async_copy(src, dst, in_sem.at[6 + i])
        for i, (src, dst) in enumerate(
            ((qrow_hbm, qrow_ref), (slot_hbm, slot_ref), (len_hbm, len_ref), (gold_hbm, gold_ref))
        )
    ]
    total = wide * narrow
    me = me_w * narrow + me_n
    far = sorted(range(1, wide), key=lambda i: (-min(i, wide - i), i))
    wides = [lax.rem(me_w + i, wide) for i in range(wide)]
    narrows = [lax.rem(me_n + i, narrow) for i in range(narrow)]
    first = me_w == 0
    patient = lax.rem(me_n, 2) == 1

    def signal(sem, to):
        pl.semaphore_signal(sem, inc=1, device_id=to, device_id_type=MESH)

    def each(low, high, fn):
        def step(i, _):
            fn(i)
            return 0
        lax.fori_loop(low, high, step, 0)

    def earlier(fn):
        each(0, me_w, fn)

    def later(fn):
        each(me_w + 1, wide, fn)

    barrier = pltpu.get_barrier_semaphore()
    later(lambda p: signal(barrier, {"wide": p}))

    @pl.when(first)
    def _():
        for to in narrows[1:]:
            signal(barrier, {"narrow": to})

    for cp in (*cp_ks, cp_v, cp_p, cp_ko, cp_vo, cp_q, *scalars):
        cp.start()

    pl.semaphore_wait(barrier, jnp.where(first, narrow - 1, me_w))
    earlier(lambda p: signal(ready.at[me_w], {"wide": p}))

    def remote(src, dst, n, to):
        return pltpu.make_async_remote_copy(
            src_ref=src, dst_ref=dst, send_sem=send_sem.at[n], recv_sem=recv_sem.at[n],
            device_id=to, device_id_type=MESH,
        )

    def share(buf, n):
        return lambda p: remote(buf.at[own], buf.at[own], n, {"wide": p}).start()

    def drained(buf, n, count):
        part = buf.at[pl.ds(0, count)]
        return remote(part, part, n, {"wide": wides[1]})

    cp_ks[0].wait()
    earlier(share(kslots[0], 4))

    cp_p.wait()
    probe = probe_ref[...]
    picks = [iota((LANES, heads), 0) % group + i * group == iota((LANES, heads), 1) for i in range(kv)]
    picks = [jnp.where(pick, 1.0, 0.0).astype(BF16) for pick in picks]
    probe_t = [jnp.dot(pick, probe, preferred_element_type=F32).astype(BF16) for pick in picks]

    def unpack(x):
        n = x.shape[0] // kv
        split[0:n * kv] = x.astype(F32)
        return [split[pl.ds(i, n, stride=kv), :] for i in range(kv)]

    cp_v.wait()
    head_kv = iota((heads, 1), 0) // group
    for r in range(quest):
        acc = jnp.zeros((heads, pref), F32)
        for i, part in enumerate(unpack(pv_v[r])):
            d = lax.dot_general(probe, part.astype(BF16), NT, preferred_element_type=F32)
            acc = jnp.where(head_kv == i, d, acc)
        vpslot[me_w * quest + r] = acc.astype(BF16)

    def meet(p):
        pl.semaphore_wait(ready.at[p], 1)
        share(vpslot, 1)(p)
        share(kslots[0], 4)(p)

    later(meet)
    earlier(share(vpslot, 1))
    for cp in cp_ks[1:]:
        cp.wait()

    def share_rest():
        def rest(p):
            for i, ref in enumerate(kslots[1:], 5):
                share(ref, i)(p)

        each(0, wide - 1 - me_w, lambda i: rest(wide - 1 - i))
        earlier(rest)

    @pl.when(jnp.logical_not(patient))
    def _():
        share_rest()

    @pl.when(first)
    def _():
        for to in narrows[1:]:
            signal(together, {"narrow": to})


    def turn(c, i, b):
        rows = q_v[c, pl.ds(b * tcols, tcols), i]
        return rows.reshape(cols, dim).T

    def absorb(s, vp, old=None, last=False):
        s = s.reshape(-1, SUBLANES, cols)
        vp = jnp.concatenate([vp] * (cols // LANES), axis=1).reshape(s.shape)
        m = jnp.max(s, axis=0)
        if old is not None:
            m = jnp.maximum(m, old[0])
        if last:
            m = jnp.max(m, axis=0, keepdims=True)
        e = jnp.exp2((s - m) * scale)
        l = jnp.sum(e, axis=0)
        n = jnp.sum(e * vp, axis=0)
        if old is not None:
            fade = jnp.exp2((old[0] - m) * scale)
            l, n = l + old[1] * fade, n + old[2] * fade
        return m, l, n

    cp_ko.wait()
    cp_vo.wait()
    cp_q.wait()
    def own_part(c, _):
        for i, x in enumerate(unpack(k_v[c])):
            kown[i] = x.astype(BF16)
        for i, x in enumerate(unpack(v_v[c])):
            vpt[i] = lax.dot_general(x.astype(BF16), probe_t[i], NT, preferred_element_type=F32)
        for at, (i, b) in enumerate(tiles):
            n_rows = (b + 1) * tcols
            qt = turn(c, i, b)
            qt_v[c, at] = qt
            s = jnp.dot(kown[i, :n_rows], qt, preferred_element_type=F32)
            ok = iota((tcols, cols), 0) <= iota((tcols, cols), 1) // group
            last = jnp.where(ok, s[n_rows - tcols:], NEG)
            s = last if b == 0 else jnp.concatenate([s[:n_rows - tcols], last], axis=0)
            ms[c, at], ls[c, at], ns[c, at] = absorb(s, vpt[i, :n_rows])
        return 0

    lax.fori_loop(0, conts, own_part, 0)

    @pl.when(first)
    def _():
        pl.semaphore_wait(together, narrow - 1)
        later(lambda p: signal(together, {"wide": p}))

    others = (wide - 1) * quest
    for cp in scalars:
        cp.wait()
    rows_of = [qrow_ref[slot_ref[c] // ANSWERS] for c in range(conts)]
    drained(vpslot, 1, others).wait_recv()

    @pl.when(patient)
    def _():
        share_rest()


    def prefix_part(part):
        at, size = chunks[part]
        keys = pl.ds(at, size)
        for c in range(conts):
            for i, x in enumerate(unpack(kslots[part][rows_of[c]])):
                kpre[c, i, keys] = x.astype(BF16)
        ratios = []
        for c in range(conts):
            below = above = jnp.ones((len(tiles), cols), F32)
            for t, (i, _) in enumerate(tiles):
                s = jnp.dot(kpre[c, i, keys], qt_v[c, t], preferred_element_type=F32)
                old = ms[c, t], ls[c, t], ns[c, t]
                if part < len(chunks) - 1:
                    ms[c, t], ls[c, t], ns[c, t] = absorb(s, vptp[c, i, keys], old)
                    continue
                _, l, n = absorb(s, vptp[c, i, keys], old, True)
                above = jnp.where(tile_id == t, jnp.sum(n, axis=0, keepdims=True), above)
                below = jnp.where(tile_id == t, jnp.sum(l, axis=0, keepdims=True), below)
            ratios.append(above / below)
        return ratios

    tile_id = iota((len(tiles), cols), 0)
    for c in range(conts):
        for i in range(kv):
            vptp[c, i] = lax.dot_general(
                vpslot[rows_of[c]], picks[i], (((0,), (1,)), ((), ())), preferred_element_type=F32
            )
    drained(kslots[0], 4, others).wait_recv()
    prefix_part(0)
    drained(kslots[1], 5, others).wait_recv()
    prefix_part(1)
    drained(kslots[2], 6, others).wait_recv()
    ratios = prefix_part(2)

    fold = jnp.where(iota((cols, clen), 0) // group == iota((cols, clen), 1) % tcols, 1.0, 0.0)
    fold = fold.astype(BF16)
    keep = iota((len(tiles), clen), 1) // tcols == iota((len(tiles), clen), 0) % blocks
    ratio = jnp.concatenate(ratios, axis=0)
    coarse = ratio.astype(BF16)
    fine = (ratio - coarse.astype(F32)).astype(BF16)
    y = jnp.dot(coarse, fold, preferred_element_type=F32)
    y = y + jnp.dot(fine, fold, preferred_element_type=F32)
    y = jnp.where(keep, y.reshape(conts, len(tiles), clen), 0.0)
    partial = jnp.sum(y, axis=1)
    tslot[me_n] = partial

    tpos = iota((1, clen), 1)
    places = iota((wide, quest * ANSWERS, 1), 0) * (quest * ANSWERS)
    places = places + iota((wide, quest * ANSWERS, 1), 1)
    term = jnp.zeros((wide, quest * ANSWERS, clen), F32)
    for c in range(conts):
        val = jnp.where(tpos < len_ref[c], partial[c:c + 1, :], 0.0)
        place = rows_of[c] * ANSWERS + slot_ref[c] % ANSWERS
        term = jnp.where(places == place, val[None], term)
    cbuf[...] = term

    @pl.when(me_w > 0)
    def _():
        pl.semaphore_wait(together, 1)

    def hand(i, j):
        to = {"wide": wides[i], "narrow": narrows[j]}
        remote(cbuf.at[wides[i]], cslot.at[me], 2, to).start()

    if total <= 16:
        for i in (*range(1, wide), 0):
            for j in range(narrow - 1, -1, -1):
                if i or j:
                    hand(i, j)
    else:
        @pl.loop(1, total)
        def _(n):
            p = lax.rem(me + n, total)
            to = {"wide": lax.div(p, narrow), "narrow": lax.rem(p, narrow)}
            remote(cbuf.at[to["wide"]], cslot.at[me], 2, to).start()

    for j in range(1, narrow):
        remote(tslot.at[me_n], tslot.at[me_n], 3, {"narrow": narrows[j]}).start()
    cslot[me] = cbuf[me_w]

    drained(tslot, 3, narrow - 1).wait_recv()
    tok = tslot[0]
    for i in range(1, narrow):
        tok = tok + tslot[i]
    out_ref[0:conts, :] = tok

    drained(cslot, 2, total - 1).wait_recv()
    drained(tslot, 3, narrow - 1).wait_send()
    drained(cslot, 2, total - 1).wait_send()
    for n, buf in ((1, vpslot), *enumerate(kslots, 4)):
        drained(buf, n, others).wait_send()
    summed = jnp.sum(jnp.sum(cslot[...], axis=0), axis=1, keepdims=True)
    logps = []
    losses = []
    for r in range(quest):
        score = summed[r * ANSWERS:(r + 1) * ANSWERS]
        top = jnp.max(score, axis=0, keepdims=True)
        norm = jnp.log(jnp.sum(jnp.exp(score - top), axis=0, keepdims=True))
        logp = score - top - norm
        gold = jnp.zeros((1, 1), jnp.int32)
        for g in range(questions):
            gold = jnp.where(me_w * quest + r == qrow_ref[g], gold_ref[g], gold)
        answer = iota((ANSWERS, LANES), 0)
        row = jnp.sum(jnp.where(answer == iota((ANSWERS, LANES), 1), logp, 0.0), axis=0, keepdims=True)
        loss = jnp.sum(jnp.where(answer == gold, -logp, 0.0), axis=0, keepdims=True)
        logps.append(row)
        losses.append(loss)
    for r in range(quest):
        out_ref[conts + r:conts + r + 1, :] = logps[r]
        out_ref[conts + quest + r:conts + quest + r + 1, :] = losses[r]


def hand_out(conts, quest, packed_ref, tok_ref, logp_ref, loss_ref):
    tok_ref[...] = packed_ref[0:conts, :]
    logp_ref[...] = packed_ref[conts:conts + quest, :ANSWERS]
    loss_ref[...] = packed_ref[conts + quest:conts + 2 * quest, :1]


def solution(mesh):
    wide, narrow = mesh.shape["wide"], mesh.shape["narrow"]
    total = wide * narrow

    def per_device(q, k, v, prefix, probe, qrow, slot, length, gold):
        conts, clen, heads, dim = q.shape
        kv = k.shape[2]
        quest, _, pref = prefix.shape[:3]
        questions = qrow.shape[0]
        cols = 2 * LANES
        tiles = clen * heads // cols
        chunks = chunks_of(pref)
        sizes = (wide, narrow, conts, clen, heads, kv, dim, quest, pref, questions)
        vmem = pl.BlockSpec(memory_space=pltpu.VMEM)
        anyw = pl.BlockSpec(memory_space=pl.ANY)
        stat = pltpu.VMEM((conts, tiles, SUBLANES, cols), F32)
        dma = pltpu.SemaphoreType.DMA
        packed = pl.pallas_call(
            functools.partial(kernel, sizes),
            out_shape=pltpu.VMEM((conts + 2 * quest, LANES), F32),
            in_specs=[anyw] * 9,
            out_specs=vmem,
            scratch_shapes=[
                pltpu.SMEM((questions,), jnp.int32),
                pltpu.SMEM((conts,), jnp.int32),
                pltpu.SMEM((conts,), jnp.int32),
                pltpu.SMEM((questions,), jnp.int32),
                pltpu.VMEM((heads, dim), BF16),
                pltpu.VMEM((conts, tiles, dim, cols), BF16),
                pltpu.VMEM((conts, clen, kv, heads // kv, dim), BF16),
                pltpu.VMEM((conts, clen * kv, dim), BF16),
                pltpu.VMEM((conts, clen * kv, dim), BF16),
                pltpu.VMEM((quest, pref * kv, dim), BF16),
                pltpu.VMEM((wide * quest, heads, pref), BF16),
                pltpu.VMEM((clen * kv, dim), F32),
                pltpu.VMEM((kv, clen, dim), BF16),
                pltpu.VMEM((kv, clen, LANES), F32),
                pltpu.VMEM((conts, kv, pref, dim), BF16),
                pltpu.VMEM((conts, kv, pref, LANES), F32),
                stat, stat, stat,
                pltpu.VMEM((narrow, conts, clen), F32),
                pltpu.VMEM((wide, quest * ANSWERS, clen), F32),
                pltpu.VMEM((total, quest * ANSWERS, clen), F32),
                dma((10 + len(chunks),)),
                dma((4 + len(chunks),)), dma((4 + len(chunks),)),
                pltpu.SemaphoreType.REGULAR((wide,)),
                pltpu.SemaphoreType.REGULAR,
                *[pltpu.VMEM((wide * quest, size * kv, dim), BF16) for _, size in chunks],
            ],
            compiler_params=pltpu.CompilerParams(collective_id=0, has_side_effects=True),
        )(
            qrow, slot, length, gold,
            q.reshape(conts, clen, kv, heads // kv, dim),
            k.reshape(conts, clen * kv, dim),
            v.reshape(conts, clen * kv, dim),
            prefix.reshape(quest, 2, pref * kv, dim),
            probe,
        )
        tok, logp, loss = pl.pallas_call(
            functools.partial(hand_out, conts, quest),
            out_shape=(
                jax.ShapeDtypeStruct((conts, clen), F32),
                jax.ShapeDtypeStruct((quest, ANSWERS), F32),
                jax.ShapeDtypeStruct((quest, 1), F32),
            ),
            in_specs=[vmem],
            out_specs=(vmem, vmem, vmem),
        )(pltpu.with_memory_space_constraint(packed, pltpu.VMEM))
        return tok, logp, loss.reshape(quest)

    return jax.shard_map(
        per_device,
        mesh=mesh,
        in_specs=(
            P(("groups", "wide"), None, "narrow", None),
            P(("groups", "wide"), None, "narrow", None),
            P(("groups", "wide"), None, "narrow", None),
            P(("groups", "wide"), None, None, "narrow", None),
            P("narrow", None),
            P("groups"),
            P(("groups", "wide")),
            P(("groups", "wide")),
            P("groups"),
        ),
        out_specs=(P(("groups", "wide"), None), P(("groups", "wide"), None), P(("groups", "wide"))),
        check_vma=False,
    )
```
